32 devices in a mesh: leaf: 8 (over y, x, core), wide: 4 (over z).
Axes of the slice: x: 2, y: 2, z: 4, core: 2. Of those that a mesh axis runs over, the one named last changes fastest.
Arguments:
- source: bfloat16 [4, 8, 4, 256, 1024], P(None, 'leaf', 'wide'), may hold values from -6 to 6
- row_factors: bfloat16 [4, 4, 8, 4, 256, 512], P(None, None, 'leaf', 'wide'), may hold values from -0.25 to 0.25
- column_factors: bfloat16 [4, 4, 8, 4, 256, 512], P(None, None, 'leaf', 'wide'), may hold values from -0.25 to 0.25
Outputs:
- result: bfloat16 [4, 8, 4, 256, 1024], P(None, 'leaf', 'wide')
The draws below stay inside these ranges and needn't reach their ends.
All inputs are finite; a program needn't handle non-finite values.
Results may differ from the reference program's by a relative error of at most 0.015.
Values may be sent and summed in bfloat16 or wider, within the bound.
A program may use at most 64 MiB of HBM per device.

```python
import jax
import jax.numpy as jnp

RANK = 256
RHS = 1024
BLK_DEV = 4
LEVELS = 4
LEAVES = 8
STRIPS = 4


def block_scale(rng, extent, shards, low, largest):
    def one(axis_at, blocks):
        heights = jax.random.uniform(jax.random.fold_in(jax.random.fold_in(rng, 6), axis_at), (blocks,), jnp.float32, low / len(shards), largest / len(shards))
        return jnp.repeat(jnp.exp(heights), extent[axis_at] // blocks).reshape((-1,) + (1,) * (len(extent) - axis_at - 1))

    gain = one(*shards[0])
    for cut in shards[1:]:
        gain = gain * one(*cut)
    return gain


def bell_draw(key, dims, deviation, bound, pieces=(), kind=jnp.bfloat16):
    factor_of = block_scale(key, dims, pieces, -0.22, 0.18) if pieces else 1.0
    array = jax.random.normal(key, dims, jnp.float32) * deviation * factor_of
    return jnp.minimum(jnp.maximum(array, -bound), bound).astype(kind)


def setup_inputs(seed: int = 0) -> dict:
    seeds = jax.random.split(jax.random.key(seed), 4)
    source = bell_draw(seeds[0], (BLK_DEV, LEAVES, STRIPS, RANK, RHS), 1.0, 6.0, ((1, 8), (2, 4)))
    row_factors = bell_draw(seeds[1], (LEVELS, BLK_DEV, LEAVES, STRIPS, RANK, 2 * RANK), (2 * RANK) ** -0.5, 0.25, ((2, 8), (3, 4)))
    column_factors = bell_draw(seeds[2], (LEVELS, BLK_DEV, LEAVES, STRIPS, RANK, 2 * RANK), (2 * RANK) ** -0.5, 0.25, ((2, 8), (3, 4)))
    return dict(source=source, row_factors=row_factors, column_factors=column_factors)


def apply_level(coeffs, factors, stride):
    groups = coeffs.shape[0]
    middle = coeffs.shape[1]
    rank_size = coeffs.shape[2]
    rhs_count = coeffs.shape[3]
    paired = coeffs.reshape(groups // (2 * stride), 2, stride, middle, rank_size, rhs_count).astype(jnp.float32)
    mats = factors.reshape(groups // (2 * stride), 2, stride, middle, rank_size, 2 * rank_size).astype(jnp.float32)
    lower_part = paired[:, 0]
    upper_part = paired[:, 1]
    result = jnp.einsum('aqsmrk,asmkh->aqsmrh', mats[..., :rank_size], lower_part)
    result = result + jnp.einsum('aqsmrk,asmkh->aqsmrh', mats[..., rank_size:], upper_part)
    return result.reshape(groups, middle, rank_size, rhs_count).astype(jnp.bfloat16)


def reference(source, row_factors, column_factors):
    coeffs = source.reshape(BLK_DEV * LEAVES, STRIPS, RANK, RHS)
    forward = row_factors.reshape(LEVELS, BLK_DEV * LEAVES, STRIPS, RANK, 2 * RANK)
    for level_no in range(LEVELS):
        coeffs = apply_level(coeffs, forward[level_no], 2 ** level_no)
    coeffs = coeffs.reshape(BLK_DEV, LEAVES, STRIPS, RANK, RHS).transpose(0, 2, 1, 3, 4)
    coeffs = coeffs.reshape(BLK_DEV * STRIPS, LEAVES, RANK, RHS)
    adjoint = column_factors.transpose(0, 1, 3, 2, 4, 5).reshape(LEVELS, BLK_DEV * STRIPS, LEAVES, RANK, 2 * RANK)
    for level_no in reversed(range(LEVELS)):
        coeffs = apply_level(coeffs, adjoint[level_no], 2 ** level_no)
    coeffs = coeffs.reshape(BLK_DEV, STRIPS, LEAVES, RANK, RHS).transpose(0, 2, 1, 3, 4)
    return coeffs
```

```python
import functools

import jax
import jax.numpy as jnp
from jax import lax
from jax.experimental import pallas as pl
from jax.experimental.pallas import tpu as pltpu
from jax.sharding import PartitionSpec as P

MESH = pl.DeviceIdType.MESH
CHUNK = 128


def make_groups(levels, sizes):
    order = [("leaf", 0, n) for n in range(levels)]
    order += [("wide", 1, n) for n in reversed(range(levels))]
    groups, pending = [], []
    for axis, which, n in order:
        stride = 1 << n
        if stride < sizes[axis]:
            groups.append(dict(axis=axis, mask=stride, slot=which * levels + n, local=[]))
        elif groups:
            groups[-1]["local"].append((stride // sizes[axis], which * levels + n))
        else:
            pending.append(n)
    assert not pending
    return groups


def kernel(groups, levels, src, row, col, out, own0, held, obuf, rcv, fac, tmp,
           src_sem, fac_sem, send_sem, recv_sem, out_sem):
    blocks, rank, _ = src.shape
    chunks = rcv.shape[1]
    count = len(groups)
    me = {a: lax.axis_index(a) for a in ("leaf", "wide")}
    bits = [lax.rem(lax.div(me[g["axis"]], g["mask"]), 2) for g in groups]
    partner = [
        {g["axis"]: me[g["axis"]] + g["mask"] * (1 - 2 * bit)} for g, bit in zip(groups, bits)
    ]

    def src_copy(k):
        cols = pl.ds(pl.multiple_of(k * CHUNK, CHUNK), CHUNK)
        return pltpu.make_async_copy(src.at[:, :, cols], own0.at[k], src_sem.at[k])

    def src_send(k):
        cols = pl.ds(pl.multiple_of(k * CHUNK, CHUNK), CHUNK)
        return pltpu.make_async_remote_copy(
            src_ref=src.at[:, :, cols], dst_ref=rcv.at[0, k], send_sem=send_sem.at[0],
            recv_sem=recv_sem.at[0, k, 0], device_id=partner[0], device_id_type=MESH)

    def fac_copies(slot, bit):
        ref = (row if slot < levels else col).at[slot % levels]
        halves = []
        for j in range(2):
            at = j * rank if bit is None else (bit if j == 0 else 1 - bit) * rank
            if bit is not None:
                at = pl.multiple_of(at, rank)
            halves.append(pltpu.make_async_copy(
                ref.at[:, :, pl.ds(at, rank)], fac.at[slot, j], fac_sem.at[slot, j]))
        return halves

    def all_fac(g):
        copies = fac_copies(groups[g]["slot"], bits[g])
        for _, slot in groups[g]["local"]:
            copies += fac_copies(slot, None)
        return copies

    def send(g, k, b):
        return pltpu.make_async_remote_copy(
            src_ref=held.at[g - 1, k, b], dst_ref=rcv.at[g, k, b], send_sem=send_sem.at[g],
            recv_sem=recv_sem.at[g, k, b], device_id=partner[g], device_id_type=MESH)

    src_copy(0).start()
    for c in all_fac(0):
        c.start()

    barrier = pltpu.get_barrier_semaphore()
    for g in range(count):
        pl.semaphore_signal(barrier, inc=1, device_id=partner[g], device_id_type=MESH)
    pl.semaphore_wait(barrier, count)

    src_send(0).start()
    for k in range(1, chunks):
        src_copy(k).start()
        src_send(k).start()
    for g in range(1, count):
        for c in all_fac(g):
            c.start()

    def mul(slot, b, first, second):
        total = jnp.dot(fac[slot, 0, b], first, preferred_element_type=jnp.float32)
        total = total + jnp.dot(fac[slot, 1, b], second, preferred_element_type=jnp.float32)
        return total.astype(jnp.bfloat16)

    def step(g, k):
        group = groups[g]

        @pl.when(k == 0)
        def _():
            for c in all_fac(g):
                c.wait()

        if g == 0:
            src_copy(k).wait()
            src_send(k).wait_recv()

        def finish(b, value):
            if g + 1 < count:
                held[g, k, b] = value
                send(g + 1, k, b).start()
            else:
                obuf[k, b] = value
                cols = pl.ds(pl.multiple_of(k * CHUNK, CHUNK), CHUNK)
                pltpu.make_async_copy(
                    obuf.at[k, b], out.at[b, :, cols], out_sem).start()

        for b in range(blocks):
            if g:
                send(g, k, b).wait_recv()
            own = own0[k, b] if g == 0 else held[g - 1, k, b]
            value = mul(group["slot"], b, own, rcv[g, k, b])
            if group["local"]:
                tmp[0, b] = value
            else:
                finish(b, value)
        for n, (stride, slot) in enumerate(group["local"]):
            now = n % 2
            for b in range(blocks):
                low = b - stride * (b // stride % 2)
                value = mul(slot, b, tmp[now, low], tmp[now, low + stride])
                if n + 1 < len(group["local"]):
                    tmp[1 - now, b] = value
                else:
                    finish(b, value)

    cut = sum(g["axis"] == "leaf" for g in groups)
    order = [0] + list(reversed(range(1, cut))) + list(range(max(cut, 1), count))

    def body(t, _):
        for g in order:
            k = t - g

            @pl.when((k >= 0) & (k < chunks))
            def _():
                step(g, k)

        return 0

    lax.fori_loop(0, chunks + count - 1, body, 0)

    pltpu.make_async_copy(own0, own0, send_sem.at[0]).wait()
    for g in range(1, count):
        pltpu.make_async_copy(held.at[g - 1], held.at[g - 1], send_sem.at[g]).wait()
    pltpu.make_async_copy(obuf, obuf, out_sem).wait()


def per_device(sizes, source, row_factors, column_factors):
    blocks, rank, rhs = source.shape[0], source.shape[3], source.shape[4]
    levels = row_factors.shape[0]
    groups = make_groups(levels, sizes)
    count = len(groups)
    chunks = rhs // CHUNK
    bf = jnp.bfloat16
    part = (chunks, blocks, rank, CHUNK)
    result = pl.pallas_call(
        functools.partial(kernel, groups, levels),
        out_shape=jax.ShapeDtypeStruct((blocks, rank, rhs), bf),
        in_specs=[pl.BlockSpec(memory_space=pl.ANY)] * 3,
        out_specs=pl.BlockSpec(memory_space=pl.ANY),
        scratch_shapes=[
            pltpu.VMEM(part, bf),
            pltpu.VMEM((count - 1,) + part, bf),
            pltpu.VMEM(part, bf),
            pltpu.VMEM((count,) + part, bf),
            pltpu.VMEM((2 * levels, 2, blocks, rank, rank), bf),
            pltpu.VMEM((2, blocks, rank, CHUNK), bf),
            pltpu.SemaphoreType.DMA((chunks,)),
            pltpu.SemaphoreType.DMA((2 * levels, 2)),
            pltpu.SemaphoreType.DMA((count,)),
            pltpu.SemaphoreType.DMA((count, chunks, blocks)),
            pltpu.SemaphoreType.DMA,
        ],
        compiler_params=pltpu.CompilerParams(
            collective_id=0, has_side_effects=True, vmem_limit_bytes=60 * 2**20),
    )(
        source.reshape(blocks, rank, rhs),
        row_factors.reshape(levels, blocks, rank, 2 * rank),
        column_factors.reshape(levels, blocks, rank, 2 * rank),
    )
    return result.reshape(source.shape)


def solution(mesh):
    return jax.shard_map(
        functools.partial(per_device, dict(mesh.shape)),
        mesh=mesh,
        in_specs=(
            P(None, "leaf", "wide", None, None),
            P(None, None, "leaf", "wide", None, None),
            P(None, None, "leaf", "wide", None, None),
        ),
        out_specs=P(None, "leaf", "wide", None, None),
        check_vma=False,
    )
```

```python
import functools

import jax
import jax.numpy as jnp
from jax import lax
from jax.experimental import pallas as pl
from jax.experimental.pallas import tpu as pltpu
from jax.sharding import PartitionSpec as P

MESH = pl.DeviceIdType.MESH
CHUNK = 128


def make_groups(levels, sizes):
    order = [("leaf", 0, n) for n in range(levels)]
    order += [("wide", 1, n) for n in reversed(range(levels))]
    groups, pending = [], []
    for axis, which, n in order:
        stride = 1 << n
        if stride < sizes[axis]:
            groups.append(dict(axis=axis, mask=stride, slot=which * levels + n, local=[]))
        elif groups:
            groups[-1]["local"].append((stride // sizes[axis], which * levels + n))
        else:
            pending.append(n)
    assert not pending
    return groups


def kernel(groups, levels, src, row, col, out, own0, held, rcv, fac, tmp,
           src_sem, fac_sem, send_sem, recv_sem):
    blocks, rank, _ = src.shape
    chunks = rcv.shape[1]
    count = len(groups)
    me = {a: lax.axis_index(a) for a in ("leaf", "wide")}
    bits = [lax.rem(lax.div(me[g["axis"]], g["mask"]), 2) for g in groups]
    partner = [
        {g["axis"]: me[g["axis"]] + g["mask"] * (1 - 2 * bit)} for g, bit in zip(groups, bits)
    ]

    def src_copy(k):
        cols = pl.ds(pl.multiple_of(k * CHUNK, CHUNK), CHUNK)
        return pltpu.make_async_copy(src.at[:, :, cols], own0.at[k], src_sem.at[k])

    def src_send(k, b):
        cols = pl.ds(pl.multiple_of(k * CHUNK, CHUNK), CHUNK)
        return pltpu.make_async_remote_copy(
            src_ref=src.at[b, :, cols], dst_ref=rcv.at[0, k, b], send_sem=send_sem.at[0],
            recv_sem=recv_sem.at[0, k, b], device_id=partner[0], device_id_type=MESH)

    def fac_copies(slot, bit):
        ref = (row if slot < levels else col).at[slot % levels]
        halves = []
        for j in range(2):
            at = j * rank if bit is None else (bit if j == 0 else 1 - bit) * rank
            if bit is not None:
                at = pl.multiple_of(at, rank)
            halves.append(pltpu.make_async_copy(
                ref.at[:, :, pl.ds(at, rank)], fac.at[slot, j], fac_sem.at[slot, j]))
        return halves

    def all_fac(g):
        copies = fac_copies(groups[g]["slot"], bits[g])
        for _, slot in groups[g]["local"]:
            copies += fac_copies(slot, None)
        return copies

    def send(g, k, b):
        return pltpu.make_async_remote_copy(
            src_ref=held.at[g - 1, k, b], dst_ref=rcv.at[g, k, b], send_sem=send_sem.at[g],
            recv_sem=recv_sem.at[g, k, b], device_id=partner[g], device_id_type=MESH)

    src_copy(0).start()
    for c in all_fac(0):
        c.start()

    barrier = pltpu.get_barrier_semaphore()
    for g in range(count):
        pl.semaphore_signal(barrier, inc=1, device_id=partner[g], device_id_type=MESH)
    pl.semaphore_wait(barrier, count)

    for b in range(blocks):
        src_send(0, b).start()
    for k in range(1, chunks):
        src_copy(k).start()
        for b in range(blocks):
            src_send(k, b).start()
    for g in range(1, count):
        for c in all_fac(g):
            c.start()

    def mul(slot, b, first, second):
        total = jnp.dot(fac[slot, 0, b], first, preferred_element_type=jnp.float32)
        total = total + jnp.dot(fac[slot, 1, b], second, preferred_element_type=jnp.float32)
        return total.astype(jnp.bfloat16)

    def step(g, k):
        group = groups[g]

        @pl.when(k == 0)
        def _():
            for c in all_fac(g):
                c.wait()

        if g == 0:
            src_copy(k).wait()

        def finish(b, value):
            if g + 1 < count:
                held[g, k, b] = value
                send(g + 1, k, b).start()
            else:
                cols = pl.ds(pl.multiple_of(k * CHUNK, CHUNK), CHUNK)
                out[b, :, cols] = value

        for b in range(blocks):
            (send(g, k, b) if g else src_send(k, b)).wait_recv()
            own = own0[k, b] if g == 0 else held[g - 1, k, b]
            value = mul(group["slot"], b, own, rcv[g, k, b])
            if group["local"]:
                tmp[0, b] = value
            else:
                finish(b, value)
        for n, (stride, slot) in enumerate(group["local"]):
            now = n % 2
            for b in range(blocks):
                low = b - stride * (b // stride % 2)
                value = mul(slot, b, tmp[now, low], tmp[now, low + stride])
                if n + 1 < len(group["local"]):
                    tmp[1 - now, b] = value
                else:
                    finish(b, value)

    cut = sum(g["axis"] == "leaf" for g in groups)
    order = [0] + list(reversed(range(1, cut))) + list(range(max(cut, 1), count))

    def body(t, _):
        for g in order:
            k = t - g

            @pl.when((k >= 0) & (k < chunks))
            def _():
                step(g, k)

        return 0

    lax.fori_loop(0, chunks + count - 1, body, 0)

    pltpu.make_async_copy(own0, own0, send_sem.at[0]).wait()
    for g in range(1, count):
        pltpu.make_async_copy(held.at[g - 1], held.at[g - 1], send_sem.at[g]).wait()


def per_device(sizes, source, row_factors, column_factors):
    blocks, rank, rhs = source.shape[0], source.shape[3], source.shape[4]
    levels = row_factors.shape[0]
    groups = make_groups(levels, sizes)
    count = len(groups)
    chunks = rhs // CHUNK
    bf = jnp.bfloat16
    part = (chunks, blocks, rank, CHUNK)
    result = pl.pallas_call(
        functools.partial(kernel, groups, levels),
        out_shape=pltpu.VMEM((blocks, rank, rhs), bf),
        in_specs=[pl.BlockSpec(memory_space=pl.ANY)] * 3,
        out_specs=pl.BlockSpec(memory_space=pltpu.VMEM),
        scratch_shapes=[
            pltpu.VMEM(part, bf),
            pltpu.VMEM((count - 1,) + part, bf),
            pltpu.VMEM((count,) + part, bf),
            pltpu.VMEM((2 * levels, 2, blocks, rank, rank), bf),
            pltpu.VMEM((2, blocks, rank, CHUNK), bf),
            pltpu.SemaphoreType.DMA((chunks,)),
            pltpu.SemaphoreType.DMA((2 * levels, 2)),
            pltpu.SemaphoreType.DMA((count,)),
            pltpu.SemaphoreType.DMA((count, chunks, blocks)),
        ],
        compiler_params=pltpu.CompilerParams(
            collective_id=0, has_side_effects=True, vmem_limit_bytes=56 * 2**20),
    )(
        source.reshape(blocks, rank, rhs),
        row_factors.reshape(levels, blocks, rank, 2 * rank),
        column_factors.reshape(levels, blocks, rank, 2 * rank),
    )
    return result.reshape(source.shape)


def solution(mesh):
    return jax.shard_map(
        functools.partial(per_device, dict(mesh.shape)),
        mesh=mesh,
        in_specs=(
            P(None, "leaf", "wide", None, None),
            P(None, None, "leaf", "wide", None, None),
            P(None, None, "leaf", "wide", None, None),
        ),
        out_specs=P(None, "leaf", "wide", None, None),
        check_vma=False,
    )
```
